32 devices in a mesh: data: 4 (over y, z), expert: 8 (over x, core).
Axes of the slice: x: 4, y: 2, z: 2, core: 2. Of those that a mesh axis runs over, the one named last changes fastest.
The devices are a block of a 4x4x8 slice.
Arguments:
- x: bfloat16 [32768, 2048], P(('data', 'expert')), parts along dimension 0
- idx: int32 [32768, 2], P(('data', 'expert')), parts along dimension 0
- wr: bfloat16 [2048, 8], replicated
- w1: bfloat16 [8, 2048, 5632], P('expert')
- w3: bfloat16 [8, 2048, 5632], P('expert')
- w2: bfloat16 [8, 5632, 2048], P('expert')
Outputs:
- output: bfloat16 [32768, 2048], P(('data', 'expert')), parts along dimension 0
There are 4 independent parts. The reference program is written for one: setup_inputs(seed, part) draws one part's arguments, and reference() takes and returns one part's arrays. A program takes and returns all parts, laid end to end along the dimension named above; an argument that names none is the same for every part.
All inputs are finite; a program needn't handle non-finite values.
Results may differ from the reference program's by a relative error of at most 0.00141.
Values are sent between devices in bfloat16 or wider.
A program may use at most 768 MiB of HBM per device.

```python
import jax
import jax.numpy as jnp
from jax import lax

N = 8
T = 1024
D = 2048
FF = 5632
TOP = 2
E = 8
CS = 512


def _routing(key):
    h = E // 2

    def one(k):
        kh, kp, ks = jax.random.split(k, 3)
        hot = jax.random.permutation(kh, E)[:h]
        p = jax.random.permutation(kp, T)
        e0 = hot[p % h]
        e1 = (e0 + 1 + (p // h) % (E - 1)) % E
        pair = jnp.stack([e0, e1], axis=1)
        swap = jax.random.bernoulli(ks, 0.5, (T, 1))
        return jnp.where(swap, pair[:, ::-1], pair)
    return jax.vmap(one)(jax.random.split(key, N)).reshape(N * T, TOP).astype(jnp.int32)


def setup_inputs(seed: int = 0, part: int = 0) -> dict:
    key = jax.random.key(seed)
    kshared, kpart = jax.random.split(key)
    kx, ki = jax.random.split(jax.random.fold_in(kpart, part))
    kr, k1, k3, k2 = jax.random.split(kshared, 4)
    x = jax.random.normal(kx, (N * T, D), jnp.float32).astype(jnp.bfloat16)
    wr = (jax.random.normal(kr, (D, E), jnp.float32) * (1.5 * D ** -0.5)).astype(jnp.bfloat16)
    w1 = (jax.random.normal(k1, (E, D, FF), jnp.float32) * D ** -0.5).astype(jnp.bfloat16)
    w3 = (jax.random.normal(k3, (E, D, FF), jnp.float32) * D ** -0.5).astype(jnp.bfloat16)
    w2 = (jax.random.normal(k2, (E, FF, D), jnp.float32) * FF ** -0.5).astype(jnp.bfloat16)
    return {'x': x, 'idx': _routing(jax.random.fold_in(ki, 7)), 'wr': wr, 'w1': w1, 'w3': w3, 'w2': w2}


def reference(x, idx, wr, w1, w3, w2):
    logits = jnp.dot(x, wr, preferred_element_type=jnp.float32)
    g = jax.nn.softmax(jnp.take_along_axis(logits, idx, axis=1), axis=-1)
    e = idx.reshape(N, T * TOP)
    oh = (e[:, :, None] == jnp.arange(E, dtype=jnp.int32)[None, None, :]).astype(jnp.int32)
    pos = jnp.take_along_axis(jnp.cumsum(oh, axis=1), e[:, :, None], axis=2)[:, :, 0] - 1
    src = jnp.arange(N, dtype=jnp.int32)[:, None]
    valid = (pos < CS).reshape(-1)
    dest = jnp.where(valid, ((e * N + src) * CS + pos).reshape(-1), E * N * CS)
    rows = jnp.repeat(x, TOP, axis=0)
    buf = jnp.zeros((E * N * CS, D), jnp.bfloat16).at[dest].set(rows, mode='drop').reshape(E, N * CS, D)

    def expert(args):
        xb, a1, a3, a2 = args
        h1 = jnp.dot(xb, a1, preferred_element_type=jnp.float32)
        h3 = jnp.dot(xb, a3, preferred_element_type=jnp.float32)
        h = (jax.nn.silu(h1) * h3).astype(jnp.bfloat16)
        return jnp.dot(h, a2, preferred_element_type=jnp.float32).astype(jnp.bfloat16)

    o = lax.map(expert, (buf, w1, w3, w2)).reshape(E * N * CS, D)
    op = jnp.where(valid[:, None], o[jnp.where(valid, dest, 0)], 0)
    y = jnp.sum(g[:, :, None] * op.reshape(N * T, TOP, D).astype(jnp.float32), axis=1)
    return y.astype(jnp.bfloat16)
```

```python
import jax
import jax.numpy as jnp
from jax import lax
from jax.experimental import pallas as pl
from jax.experimental.pallas import tpu as pltpu
from jax.sharding import PartitionSpec as P


VMEM_LIMIT = 67043328
TT = 128


def _params():
    return pltpu.CompilerParams(vmem_limit_bytes=VMEM_LIMIT)


def _dispatch(pos_or_idx, ecol, x, cap, offs, gate=None):
    first = gate is None
    t, d = x.shape
    m = ecol.shape[0]
    bf = jnp.bfloat16

    def kernel(p_ref, e_ref, x_ref, *refs):
        if first:
            pos_ref, beg_ref, *refs = refs
            e = e_ref[...]
            oh = (p_ref[0:1, :] == e) | (p_ref[1:2, :] == e)
            a = lax.broadcasted_iota(jnp.int32, (t, t), 0)
            b = lax.broadcasted_iota(jnp.int32, (t, t), 1)
            tri = jnp.where(a < b, 1.0, 0.0).astype(bf)
            ohb = jnp.where(oh, 1.0, 0.0).astype(bf)
            cnt = jnp.dot(ohb, tri, preferred_element_type=jnp.float32).astype(jnp.int32)
            pos = jnp.where(oh, cnt, -1)
            pos_ref[...] = pos
            ti = lax.broadcasted_iota(jnp.int32, (t, 128), 0)
            tj = lax.broadcasted_iota(jnp.int32, (t, 128), 1) * TT
            before = jnp.where(ti < tj, 1.0, 0.0).astype(bf)
            beg_ref[...] = jnp.dot(ohb, before, preferred_element_type=jnp.float32).astype(jnp.int32)
        else:
            idx_ref, wr_ref, erow_ref, post_ref, g_ref, *refs = refs
            pos = p_ref[...]
            post_ref[...] = pos.T
            logits = jnp.dot(x_ref[...], wr_ref[...], preferred_element_type=jnp.float32)
            ids = lax.broadcasted_iota(jnp.int32, logits.shape, 1)
            i0, i1 = idx_ref[:, 0:1], idx_ref[:, 1:2]
            s0 = jnp.sum(jnp.where(i0 == ids, logits, 0.0), axis=1, keepdims=True)
            s1 = jnp.sum(jnp.where(i1 == ids, logits, 0.0), axis=1, keepdims=True)
            top = jnp.maximum(s0, s1)
            p0, p1 = jnp.exp(s0 - top), jnp.exp(s1 - top)
            den = p0 + p1
            er = erow_ref[...]
            g_ref[...] = jnp.where(i0 == er, p0 / den, jnp.where(i1 == er, p1 / den, 0.0))
        outs, (dm_ref, st_ref, sem) = refs[:-3], refs[-3:]
        over = jnp.max(pos, axis=(0, 1), keepdims=True) >= cap - 1
        flag = jnp.where(over, 1.0, 0.0)
        r = lax.broadcasted_iota(jnp.int32, (cap, t), 0)
        last = lax.broadcasted_iota(jnp.int32, (16, 128), 0) == 15
        copies = []
        for i, o in enumerate(offs):
            slot = i % 2
            if i >= 2:
                copies[i - 2].wait()
            p = pos[o:o + 1, :]
            dm_ref[...] = jnp.where(r == jnp.where(p < cap - 1, p, -1), 1.0, 0.0).astype(bf)
            st_ref[slot] = jnp.dot(dm_ref[...], x_ref[...], preferred_element_type=jnp.float32).astype(bf)
            tail = st_ref[slot, cap - 16:cap, 0:128].astype(jnp.float32)
            st_ref[slot, cap - 16:cap, 0:128] = jnp.where(last, flag, tail).astype(bf)
            copies.append(pltpu.make_async_copy(st_ref.at[slot], outs[i], sem.at[slot]))
            copies[i].start()
        for c in copies[-2:]:
            c.wait()

    vm = pl.BlockSpec(memory_space=pltpu.VMEM)
    hbm = pl.BlockSpec(memory_space=pl.ANY)
    shapes = [jax.ShapeDtypeStruct((cap, d), bf) for _ in offs]
    specs = [hbm] * len(offs)
    if first:
        shapes = [jax.ShapeDtypeStruct((m, t), jnp.int32), jax.ShapeDtypeStruct((m, 128), jnp.int32)] + shapes
        specs = [vm] * 2 + specs
        extra = []
    else:
        shapes = [jax.ShapeDtypeStruct((t, m), jnp.int32), jax.ShapeDtypeStruct((t, m), jnp.float32)] + shapes
        specs = [vm] * 2 + specs
        extra = list(gate)
    return pl.pallas_call(
        kernel,
        in_specs=[vm] * (3 + len(extra)),
        out_specs=specs,
        out_shape=shapes,
        scratch_shapes=[pltpu.VMEM((cap, t), bf), pltpu.VMEM((2, cap, d), bf), pltpu.SemaphoreType.DMA((2,))],
        compiler_params=_params(),
        cost_estimate=pl.CostEstimate(flops=2 * len(offs) * cap * t * d, bytes_accessed=2 * d * (t + len(offs) * cap), transcendentals=0),
    )(pos_or_idx, ecol, x, *extra)


def _ffn(blocks, prev, w1, w3, w2):
    nb = len(blocks)
    cap, d = blocks[0].shape
    ff = w1.shape[-1]
    ft, nt = 512, 256
    s1, s2 = (3, 3) if nb * cap < 512 else (2, 2)
    n1, n2 = ff // ft, d // nt
    bf = jnp.bfloat16

    def kernel(*refs):
        xs = refs[:nb]
        pf_ref, w1h, w3h, w2h = refs[nb:nb + 4]
        os = refs[nb + 4:2 * nb + 4]
        fl_ref, h_ref, wa, wc, xv, ov, sa, sb, sc, sx, so = refs[2 * nb + 4:]

        def c1(i, slot):
            cols = pl.ds(pl.multiple_of(i * ft, ft), ft)
            return (pltpu.make_async_copy(w1h.at[0, :, cols], wa.at[slot, :, 0:ft], sa.at[slot]),
                    pltpu.make_async_copy(w3h.at[0, :, cols], wa.at[slot, :, ft:2 * ft], sb.at[slot]))

        def c2(i, slot):
            cols = pl.ds(pl.multiple_of(i * nt, nt), nt)
            return pltpu.make_async_copy(w2h.at[0, :, cols], wc.at[slot], sc.at[slot])

        def oc(i, q, slot):
            cols = pl.ds(pl.multiple_of(i * nt, nt), nt)
            return pltpu.make_async_copy(ov.at[slot, pl.ds(q * cap, cap)], os[q].at[:, cols], so.at[slot, q])

        cx = [pltpu.make_async_copy(xs[q], xv.at[pl.ds(q * cap, cap)], sx.at[q]) for q in range(nb)]
        for c in (cx[0], *c1(0, 0), *cx[1:]):
            c.start()
        for c in (*cx, *c1(0, 0)):
            c.wait()
        for s in range(1, s1):
            for c in c1(s, s):
                c.start()

        def step1(i, _):
            slot = lax.rem(i, s1)

            @pl.when(i > 0)
            def _():
                for c in c1(i, slot):
                    c.wait()

            for s in range(s2):
                @pl.when(i == n1 - 2 * s2 + 2 * s - 1)
                def _():
                    c2(s, s).start()
            ab = jnp.dot(xv[...], wa[slot], preferred_element_type=jnp.float32)
            a, b = ab[:, :ft], ab[:, ft:]
            h_ref[:, pl.ds(pl.multiple_of(i * ft, ft), ft)] = (jax.nn.silu(a) * b).astype(bf)

            @pl.when(i + s1 < n1)
            def _():
                for c in c1(i + s1, slot):
                    c.start()

            return 0

        lax.fori_loop(0, n1, step1, 0)

        def step2(i, _):
            slot = lax.rem(i, s2)
            oslot = lax.rem(i, 2)
            c2(i, slot).wait()

            @pl.when(i >= 2)
            def _():
                for q in range(nb):
                    oc(i - 2, q, oslot).wait()

            ov[oslot] = jnp.dot(h_ref[...], wc[slot], preferred_element_type=jnp.float32).astype(bf)
            for q in range(nb):
                oc(i, q, oslot).start()

            @pl.when(i + s2 < n2)
            def _():
                c2(i + s2, slot).start()

            return 0

        lax.fori_loop(0, n2, step2, 0)
        fl = pf_ref[...]
        row = lax.broadcasted_iota(jnp.int32, (16, 128), 0)
        for q in range(nb):
            tail = xv[(q + 1) * cap - 16:(q + 1) * cap, 0:128].astype(jnp.float32)
            fl = jnp.maximum(fl, jnp.max(jnp.where(row == 15, tail, 0.0), axis=0, keepdims=True))
        fl_ref[...] = fl
        for i in (n2 - 2, n2 - 1):
            for q in range(nb):
                oc(i, q, i % 2).wait()

    hbm = pl.BlockSpec(memory_space=pl.ANY)
    vm = pl.BlockSpec(memory_space=pltpu.VMEM)
    return pl.pallas_call(
        kernel,
        in_specs=[hbm] * nb + [vm] + [hbm] * 3,
        out_specs=[hbm] * nb + [vm],
        out_shape=[jax.ShapeDtypeStruct((cap, d), bf)] * nb + [jax.ShapeDtypeStruct((8, 128), jnp.float32)],
        scratch_shapes=[
            pltpu.VMEM((nb * cap, ff), bf),
            pltpu.VMEM((s1, d, 2 * ft), bf),
            pltpu.VMEM((s2, ff, nt), bf),
            pltpu.VMEM((nb * cap, d), bf),
            pltpu.VMEM((2, nb * cap, nt), bf),
            pltpu.SemaphoreType.DMA((s1,)),
            pltpu.SemaphoreType.DMA((s1,)),
            pltpu.SemaphoreType.DMA((s2,)),
            pltpu.SemaphoreType.DMA((nb,)),
            pltpu.SemaphoreType.DMA((2, nb)),
        ],
        compiler_params=_params(),
        cost_estimate=pl.CostEstimate(flops=6 * nb * cap * d * ff, bytes_accessed=6 * d * ff, transcendentals=nb * cap * ff),
    )(*blocks, prev, w1, w3, w2)


def _combine(blocks, pos, beg, g, extra, dtype):
    nb = len(blocks)
    cap, d = blocks[0].shape
    t = pos.shape[0]
    nt = 256
    win = TT + 16
    bf = jnp.bfloat16

    def kernel(beg_ref, pos_ref, g_ref, *refs):
        bs = refs[:nb]
        x_ref = refs[nb] if extra is not None else None
        y_ref, s_ref = refs[-2:]

        def first_row(i, o):
            return pl.multiple_of(jnp.minimum(beg_ref[o, i] // 16 * 16, cap - win), 16)

        @pl.when(pl.program_id(0) == 0)
        def _():
            r = lax.broadcasted_iota(jnp.int32, (TT, win), 1)
            for i in range(t // TT):
                for o in range(nb):
                    p = pos_ref[i * TT:(i + 1) * TT, o:o + 1]
                    p = jnp.where(p < cap - 1, p - first_row(i, o), -1)
                    s_ref[i, o] = jnp.where(r == p, 1.0, 0.0).astype(bf)

        for i in range(t // TT):
            rows = slice(i * TT, (i + 1) * TT)
            acc = x_ref[rows, :] if x_ref is not None else None
            for o in range(nb):
                v = jnp.dot(s_ref[i, o], bs[o][pl.ds(first_row(i, o), win), :], preferred_element_type=jnp.float32)
                v = v * g_ref[rows, o:o + 1]
                acc = v if acc is None else acc + v
            y_ref[rows, :] = acc.astype(dtype)

    small = pl.BlockSpec(pos.shape, lambda i: (0, 0))
    bsp = pl.BlockSpec((cap, nt), lambda i: (0, i))
    ysp = pl.BlockSpec((t, nt), lambda i: (0, i))
    args = [beg, pos, g, *blocks] + ([extra] if extra is not None else [])
    return pl.pallas_call(
        kernel,
        grid=(d // nt,),
        in_specs=[pl.BlockSpec(memory_space=pltpu.SMEM), small, small] + [bsp] * nb + ([ysp] if extra is not None else []),
        out_specs=ysp,
        out_shape=jax.ShapeDtypeStruct((t, d), dtype),
        scratch_shapes=[pltpu.VMEM((t // TT, nb, TT, win), bf)],
        compiler_params=_params(),
        cost_estimate=pl.CostEstimate(flops=2 * nb * 256 * t * d, bytes_accessed=2 * nb * cap * d + 8 * t * d, transcendentals=0),
    )(*args)


def solution(mesh):
    n = mesh.shape['expert']
    chips = n // 2
    offsets = [(dc, f) for dc in range(chips) for f in range(2)]

    def target(s, o):
        dc, f = offsets[o]
        return ((s // 2 + dc) % chips) * 2 + (s % 2) * (1 - 2 * f) + f

    out_perm = [[(s, target(s, o)) for s in range(n)] for o in range(n)]
    back_perm = [[(b, a) for a, b in p] for p in out_perm]

    order = sorted((o for o in range(n) if offsets[o][0]), key=lambda o: (offsets[o][0] == chips // 2, offsets[o][1]))
    near = [o for o in order if offsets[o][0] != chips // 2]
    far = [o for o in order if offsets[o][0] == chips // 2]
    steps = [[0], near[:2], far, near[2:], [1]]

    def local(x, idx, wr, w1, w3, w2):
        t, _ = x.shape
        k = idx.shape[1]
        e_all = wr.shape[1]
        cs = 2 * k * t // e_all
        cap = cs * 23 // 32
        me = lax.axis_index('expert')
        eoff = jnp.stack([target(me, o) for o in range(n)]).astype(jnp.int32)

        ecol = eoff[:, None]
        send = [None] * n
        first = near[:2] + [0]
        pos, beg, *b = _dispatch(idx.T, ecol, x, cap, first)
        for o, v in zip(first, b):
            send[o] = v

        def move(v, o, perm):
            return lax.ppermute(v, 'expert', perm[o])

        recv = list(send)
        back = [None] * n
        fl = jnp.zeros((8, 128), jnp.float32)
        for o in near[:2]:
            recv[o] = move(send[o], o, out_perm)
        for i, offs in enumerate(steps):
            *outs, fl = _ffn([recv[o] for o in offs], fl, w1, w3, w2)
            for o, v in zip(offs, outs):
                back[o] = v if o == 0 else move(v, o, back_perm)
            if i == 0:
                rest = far + near[2:] + [1]
                pos, _ = lax.optimization_barrier([pos, fl])
                post, g, *c = _dispatch(pos, ecol, x, cap, rest, (idx, wr, eoff[None, :]))
                for o, v in zip(rest, c):
                    send[o] = v
                for o in far + [1]:
                    recv[o] = move(send[o], o, out_perm)
            if i == 1:
                *ins, _ = lax.optimization_barrier([send[o] for o in near[2:]] + [fl])
                for o, v in zip(near[2:], ins):
                    recv[o] = move(v, o, out_perm)

        over = fl[0, 0] > 0

        def fast(back, pos, beg, g, *_):
            return _combine(back, pos, beg, g, None, x.dtype)

        def slow(back, pos, beg, g, x, eoff, w1, w3, w2):
            low = (cap - 1) // 32 * 32
            ext = cs - low
            rows = e_all * ext
            q = jnp.where((pos >= cap - 1) & (pos < cs), eoff[None, :] * ext + pos - low, rows)
            r = jnp.arange(rows, dtype=jnp.int32)
            dm = jnp.any(r[:, None, None] == q[None], axis=2).astype(x.dtype)
            sb = jnp.dot(dm, x, preferred_element_type=x.dtype)
            rb = lax.all_to_all(sb, 'expert', 0, 0, tiled=True)
            ob, _ = _ffn([rb], jnp.zeros((8, 128), jnp.float32), w1, w3, w2)
            bk = lax.all_to_all(ob, 'expert', 0, 0, tiled=True)
            tail = 0.0
            for o in range(n):
                sel = (q[:, o][:, None] == r[None, :]).astype(x.dtype)
                tail = tail + g[:, o:o + 1] * jnp.dot(sel, bk, preferred_element_type=jnp.float32)
            return _combine(back, pos, beg, g, tail, x.dtype)

        return lax.cond(over, slow, fast, back, post, beg, g, x, eoff, w1, w3, w2)

    tok = P(('data', 'expert'), None)
    wsp = P('expert', None, None)

    return jax.shard_map(local, mesh=mesh, in_specs=(tok, tok, P(), wsp, wsp, wsp), out_specs=tok, check_vma=False)
```

```python
import jax
import jax.numpy as jnp
from jax import lax
from jax.experimental import pallas as pl
from jax.experimental.pallas import tpu as pltpu
from jax.sharding import PartitionSpec as P


VMEM_LIMIT = 67043328
TT = 128


def _params():
    return pltpu.CompilerParams(vmem_limit_bytes=VMEM_LIMIT)


def _dispatch(pos_or_idx, ecol, x, cap, offs, gate=None):
    first = gate is None
    t, d = x.shape
    m = ecol.shape[0]
    bf = jnp.bfloat16

    def kernel(p_ref, e_ref, x_ref, *refs):
        if first:
            pos_ref, beg_ref, *refs = refs
            e = e_ref[...]
            oh = (p_ref[0:1, :] == e) | (p_ref[1:2, :] == e)
            a = lax.broadcasted_iota(jnp.int32, (t, t), 0)
            b = lax.broadcasted_iota(jnp.int32, (t, t), 1)
            tri = jnp.where(a < b, 1.0, 0.0).astype(bf)
            ohb = jnp.where(oh, 1.0, 0.0).astype(bf)
            cnt = jnp.dot(ohb, tri, preferred_element_type=jnp.float32).astype(jnp.int32)
            pos = jnp.where(oh, cnt, -1)
            pos_ref[...] = pos
            ti = lax.broadcasted_iota(jnp.int32, (t, 128), 0)
            tj = lax.broadcasted_iota(jnp.int32, (t, 128), 1) * TT
            before = jnp.where(ti < tj, 1.0, 0.0).astype(bf)
            beg_ref[...] = jnp.dot(ohb, before, preferred_element_type=jnp.float32).astype(jnp.int32)
        else:
            idx_ref, wr_ref, post_ref, g_ref, *refs = refs
            pos = p_ref[...]
            post_ref[...] = pos.T
            logits = lax.dot_general(wr_ref[...], x_ref[...], (((1,), (1,)), ((), ())), preferred_element_type=jnp.float32)
            ids = lax.broadcasted_iota(jnp.int32, logits.shape, 0)
            i0, i1 = idx_ref[0:1, :], idx_ref[1:2, :]
            s0 = jnp.sum(jnp.where(i0 == ids, logits, 0.0), axis=0, keepdims=True)
            s1 = jnp.sum(jnp.where(i1 == ids, logits, 0.0), axis=0, keepdims=True)
            top = jnp.maximum(s0, s1)
            p0, p1 = jnp.exp(s0 - top), jnp.exp(s1 - top)
            den = p0 + p1
            e = e_ref[...]
            g_ref[...] = jnp.where(i0 == e, p0 / den, jnp.where(i1 == e, p1 / den, 0.0)).T
        outs, (dm_ref, st_ref, posm_ref, sem) = refs[:-4], refs[-4:]
        over = jnp.max(pos, axis=(0, 1), keepdims=True) >= cap - 1
        flag = jnp.where(over, 1.0, 0.0)
        r = lax.broadcasted_iota(jnp.int32, (cap, t), 0)
        last = lax.broadcasted_iota(jnp.int32, (16, 128), 0) == 15

        def copy(i, slot):
            return pltpu.make_async_copy(st_ref.at[slot], outs[i], sem.at[slot])

        posm_ref[...] = jnp.where(pos < cap - 1, pos, -1)

        def block(i, _):
            slot = lax.rem(i, 2)
            o = offs[-1]
            for j in range(len(offs) - 1):
                o = jnp.where(i == j, offs[j], o)
            dm_ref[...] = jnp.where(r == posm_ref[pl.ds(o, 1), :], 1.0, 0.0).astype(bf)

            @pl.when(i >= 2)
            def _():
                copy(0, slot).wait()

            st_ref[slot] = jnp.dot(dm_ref[...], x_ref[...], preferred_element_type=jnp.float32).astype(bf)
            tail = st_ref[slot, cap - 16:cap, 0:128].astype(jnp.float32)
            st_ref[slot, cap - 16:cap, 0:128] = jnp.where(last, flag, tail).astype(bf)
            for j in range(len(offs)):
                @pl.when(i == j)
                def _():
                    copy(j, slot).start()
            return 0

        lax.fori_loop(0, len(offs), block, 0)
        for i in range(max(len(offs) - 2, 0), len(offs)):
            copy(i, i % 2).wait()

    vm = pl.BlockSpec(memory_space=pltpu.VMEM)
    hbm = pl.BlockSpec(memory_space=pl.ANY)
    shapes = [jax.ShapeDtypeStruct((cap, d), bf) for _ in offs]
    specs = [hbm] * len(offs)
    if first:
        shapes = [jax.ShapeDtypeStruct((m, t), jnp.int32), jax.ShapeDtypeStruct((m, 128), jnp.int32)] + shapes
        specs = [vm] * 2 + specs
        extra = []
    else:
        shapes = [jax.ShapeDtypeStruct((t, m), jnp.int32), jax.ShapeDtypeStruct((t, m), jnp.float32)] + shapes
        specs = [vm] * 2 + specs
        extra = list(gate)
    return pl.pallas_call(
        kernel,
        in_specs=[vm] * (3 + len(extra)),
        out_specs=specs,
        out_shape=shapes,
        scratch_shapes=[pltpu.VMEM((cap, t), bf), pltpu.VMEM((2, cap, d), bf), pltpu.VMEM((m, t), jnp.int32), pltpu.SemaphoreType.DMA((2,))],
        compiler_params=_params(),
        cost_estimate=pl.CostEstimate(flops=2 * len(offs) * cap * t * d, bytes_accessed=2 * d * (t + len(offs) * cap), transcendentals=0),
    )(pos_or_idx, ecol, x, *extra)


def _ffn(blocks, prev, w1, w3, w2):
    nb = len(blocks)
    cap, d = blocks[0].shape
    ff = w1.shape[-1]
    ft, nt = 512, 256
    s1, s2 = (3, 3) if nb * cap < 512 else (2, 2)
    n1, n2 = ff // ft, d // nt
    bf = jnp.bfloat16

    def kernel(*refs):
        xs = refs[:nb]
        pf_ref, w1h, w3h, w2h = refs[nb:nb + 4]
        os = refs[nb + 4:2 * nb + 4]
        fl_ref, h_ref, wa, wc, xv, ov, sa, sb, sc, sx, so = refs[2 * nb + 4:]

        def c1(i, slot):
            cols = pl.ds(pl.multiple_of(i * ft, ft), ft)
            return (pltpu.make_async_copy(w1h.at[0, :, cols], wa.at[slot, :, 0:ft], sa.at[slot]),
                    pltpu.make_async_copy(w3h.at[0, :, cols], wa.at[slot, :, ft:2 * ft], sb.at[slot]))

        def c2(i, slot):
            cols = pl.ds(pl.multiple_of(i * nt, nt), nt)
            return pltpu.make_async_copy(w2h.at[0, :, cols], wc.at[slot], sc.at[slot])

        def oc(i, q, slot):
            cols = pl.ds(pl.multiple_of(i * nt, nt), nt)
            return pltpu.make_async_copy(ov.at[slot, pl.ds(q * cap, cap)], os[q].at[:, cols], so.at[slot, q])

        cx = [pltpu.make_async_copy(xs[q], xv.at[pl.ds(q * cap, cap)], sx.at[q]) for q in range(nb)]
        for c in (cx[0], *c1(0, 0), *cx[1:]):
            c.start()
        for c in (*cx, *c1(0, 0)):
            c.wait()
        for s in range(1, s1):
            for c in c1(s, s):
                c.start()

        def step1(i, _):
            slot = lax.rem(i, s1)

            @pl.when(i > 0)
            def _():
                for c in c1(i, slot):
                    c.wait()

            for s in range(s2):
                @pl.when(i == n1 - 2 * s2 + 2 * s - 1)
                def _():
                    c2(s, s).start()
            ab = jnp.dot(xv[...], wa[slot], preferred_element_type=jnp.float32)
            a, b = ab[:, :ft], ab[:, ft:]
            h_ref[:, pl.ds(pl.multiple_of(i * ft, ft), ft)] = (jax.nn.silu(a) * b).astype(bf)

            @pl.when(i + s1 < n1)
            def _():
                for c in c1(i + s1, slot):
                    c.start()

            return 0

        lax.fori_loop(0, n1, step1, 0)

        def step2(i, _):
            slot = lax.rem(i, s2)
            oslot = lax.rem(i, 2)
            c2(i, slot).wait()

            @pl.when(i >= 2)
            def _():
                for q in range(nb):
                    oc(i - 2, q, oslot).wait()

            ov[oslot] = jnp.dot(h_ref[...], wc[slot], preferred_element_type=jnp.float32).astype(bf)
            for q in range(nb):
                oc(i, q, oslot).start()

            @pl.when(i + s2 < n2)
            def _():
                c2(i + s2, slot).start()

            return 0

        lax.fori_loop(0, n2, step2, 0)
        fl = pf_ref[...]
        row = lax.broadcasted_iota(jnp.int32, (16, 128), 0)
        for q in range(nb):
            tail = xv[(q + 1) * cap - 16:(q + 1) * cap, 0:128].astype(jnp.float32)
            fl = jnp.maximum(fl, jnp.max(jnp.where(row == 15, tail, 0.0), axis=0, keepdims=True))
        fl_ref[...] = fl
        for i in (n2 - 2, n2 - 1):
            for q in range(nb):
                oc(i, q, i % 2).wait()

    hbm = pl.BlockSpec(memory_space=pl.ANY)
    vm = pl.BlockSpec(memory_space=pltpu.VMEM)
    return pl.pallas_call(
        kernel,
        in_specs=[hbm] * nb + [vm] + [hbm] * 3,
        out_specs=[hbm] * nb + [vm],
        out_shape=[jax.ShapeDtypeStruct((cap, d), bf)] * nb + [jax.ShapeDtypeStruct((8, 128), jnp.float32)],
        scratch_shapes=[
            pltpu.VMEM((nb * cap, ff), bf),
            pltpu.VMEM((s1, d, 2 * ft), bf),
            pltpu.VMEM((s2, ff, nt), bf),
            pltpu.VMEM((nb * cap, d), bf),
            pltpu.VMEM((2, nb * cap, nt), bf),
            pltpu.SemaphoreType.DMA((s1,)),
            pltpu.SemaphoreType.DMA((s1,)),
            pltpu.SemaphoreType.DMA((s2,)),
            pltpu.SemaphoreType.DMA((nb,)),
            pltpu.SemaphoreType.DMA((2, nb)),
        ],
        compiler_params=_params(),
        cost_estimate=pl.CostEstimate(flops=6 * nb * cap * d * ff, bytes_accessed=6 * d * ff, transcendentals=nb * cap * ff),
    )(*blocks, prev, w1, w3, w2)


def _combine(blocks, pos, beg, g, extra, dtype, base, low, high):
    nb = len(blocks)
    cap, d = blocks[0].shape
    t = pos.shape[0]
    nt = 256
    win = TT + 16
    bf = jnp.bfloat16

    def kernel(beg_ref, pos_ref, g_ref, *refs):
        bs = refs[:nb]
        x_ref = refs[nb] if extra is not None else None
        y_ref, s_ref = refs[-2:]

        def first_row(i, o):
            return pl.multiple_of(jnp.clip((beg_ref[o, i] - base) // 16 * 16, 0, cap - win), 16)

        @pl.when(pl.program_id(0) == 0)
        def _():
            r = lax.broadcasted_iota(jnp.int32, (TT, win), 1)

            @pl.loop(0, t // TT)
            def _(i):
                ps = pos_ref[pl.ds(pl.multiple_of(i * TT, TT), TT), :]
                for o in range(nb):
                    p = ps[:, o:o + 1]
                    p = jnp.where((p >= low) & (p < high), p - base - first_row(i, o), -1)
                    s_ref[i, o] = jnp.where(r == p, 1.0, 0.0).astype(bf)

        for i in range(t // TT):
            rows = slice(i * TT, (i + 1) * TT)
            acc = x_ref[rows, :] if x_ref is not None else None
            for o in range(nb):
                v = jnp.dot(s_ref[i, o], bs[o][pl.ds(first_row(i, o), win), :], preferred_element_type=jnp.float32)
                v = v * g_ref[rows, o:o + 1]
                acc = v if acc is None else acc + v
            y_ref[rows, :] = acc.astype(dtype)

    small = pl.BlockSpec(pos.shape, lambda i: (0, 0))
    bsp = pl.BlockSpec((cap, nt), lambda i: (0, i))
    ysp = pl.BlockSpec((t, nt), lambda i: (0, i))
    args = [beg, pos, g, *blocks] + ([extra] if extra is not None else [])
    return pl.pallas_call(
        kernel,
        grid=(d // nt,),
        in_specs=[pl.BlockSpec(memory_space=pltpu.SMEM), small, small] + [bsp] * nb + ([ysp] if extra is not None else []),
        out_specs=ysp,
        out_shape=jax.ShapeDtypeStruct((t, d), dtype),
        scratch_shapes=[pltpu.VMEM((t // TT, nb, TT, win), bf)],
        compiler_params=_params(),
        cost_estimate=pl.CostEstimate(flops=2 * nb * 256 * t * d, bytes_accessed=2 * nb * cap * d + 8 * t * d, transcendentals=0),
    )(*args)


def solution(mesh):
    n = mesh.shape['expert']
    chips = n // 2
    offsets = [(dc, f) for dc in range(chips) for f in range(2)]

    def target(s, o):
        dc, f = offsets[o]
        return ((s // 2 + dc) % chips) * 2 + (s % 2) * (1 - 2 * f) + f

    out_perm = [[(s, target(s, o)) for s in range(n)] for o in range(n)]
    back_perm = [[(b, a) for a, b in p] for p in out_perm]

    order = sorted((o for o in range(n) if offsets[o][0]), key=lambda o: (offsets[o][0] == chips // 2, offsets[o][1]))
    near = [o for o in order if offsets[o][0] != chips // 2]
    far = [o for o in order if offsets[o][0] == chips // 2]
    steps = [[0], near[:2], far, near[2:], [1]]

    def local(x, idx, wr, w1, w3, w2):
        t, d = x.shape
        k = idx.shape[1]
        e_all = wr.shape[1]
        cs = 2 * k * t // e_all
        cap = cs * 23 // 32
        me = lax.axis_index('expert')
        eoff = jnp.stack([target(me, o) for o in range(n)]).astype(jnp.int32)

        ecol = eoff[:, None]
        send = [None] * n
        first = near[:2] + [0]
        pos, beg, *b = _dispatch(idx.T, ecol, x, cap, first)
        for o, v in zip(first, b):
            send[o] = v

        def move(v, o, perm):
            return lax.ppermute(v, 'expert', perm[o])

        recv = list(send)
        back = [None] * n
        fl = jnp.zeros((8, 128), jnp.float32)
        for o in near[:2]:
            recv[o] = move(send[o], o, out_perm)
        for i, offs in enumerate(steps):
            *outs, fl = _ffn([recv[o] for o in offs], fl, w1, w3, w2)
            for o, v in zip(offs, outs):
                back[o] = v if o == 0 else move(v, o, back_perm)
            if i == 0:
                rest = far + near[2:] + [1]
                pos, _ = lax.optimization_barrier([pos, fl])
                post, g, *c = _dispatch(pos, ecol, x, cap, rest, (idx.T, wr.T))
                for o, v in zip(rest, c):
                    send[o] = v
                for o in far + [1]:
                    recv[o] = move(send[o], o, out_perm)
            if i == 1:
                *ins, _ = lax.optimization_barrier([send[o] for o in near[2:]] + [fl])
                for o, v in zip(near[2:], ins):
                    recv[o] = move(v, o, out_perm)

        over = fl[0, 0] > 0

        def fast(back, pos, beg, g, *_):
            return _combine(back, pos, beg, g, None, x.dtype, 0, 0, cap - 1)

        def slow(back, pos, beg, g, x, eoff, w1, w3, w2):
            low = (cap - 1) // 32 * 32
            ext = cs - low
            rows = e_all * ext
            q = jnp.where((pos >= cap - 1) & (pos < cs), eoff[None, :] * ext + pos - low, rows)
            r = jnp.arange(rows, dtype=jnp.int32)
            dm = jnp.any(r[:, None, None] == q[None], axis=2).astype(x.dtype)
            sb = jnp.dot(dm, x, preferred_element_type=x.dtype)
            rb = lax.all_to_all(sb, 'expert', 0, 0, tiled=True)
            zero = jnp.zeros((8, 128), jnp.float32)
            ob = lax.map(lambda v: _ffn([v], zero, w1, w3, w2)[0], rb.reshape(n, ext, d))
            bk = lax.all_to_all(ob.reshape(rows, d), 'expert', 0, 0, tiled=True).reshape(n, ext, d)
            tail = [lax.dynamic_index_in_dim(bk, eoff[o], 0, keepdims=False) for o in range(n)]
            tail = _combine(tail, pos, beg, g, None, jnp.float32, low, cap - 1, cs)
            return _combine(back, pos, beg, g, tail, x.dtype, 0, 0, cap - 1)

        return lax.cond(over, slow, fast, back, post, beg, g, x, eoff, w1, w3, w2)

    tok = P(('data', 'expert'), None)
    wsp = P('expert', None, None)

    return jax.shard_map(local, mesh=mesh, in_specs=(tok, tok, P(), wsp, wsp, wsp), out_specs=tok, check_vma=False)
```
